16 devices in a mesh: rep: 4 (over y, z, core), pp: 4 (over x).
Axes of the slice: x: 4, y: 2, z: 1, core: 2. Of those that a mesh axis runs over, the one named last changes fastest.
The devices are a block of a 4x4x8 slice.
Arguments:
- x: bfloat16 [32, 512, 512], P('rep'), parts along dimension 0
- dy: bfloat16 [32, 512, 512], P('rep'), parts along dimension 0
- w_gate: bfloat16 [4, 512, 1280], P('pp')
- w_up: bfloat16 [4, 512, 1280], P('pp')
- w_down: bfloat16 [4, 1280, 512], P('pp')
Outputs:
- output 1: bfloat16 [16, 512, 1280], P(('rep', 'pp')), parts along dimension 0
- output 2: bfloat16 [16, 512, 1280], P(('rep', 'pp')), parts along dimension 0
- output 3: bfloat16 [16, 1280, 512], P(('rep', 'pp')), parts along dimension 0
There are 4 independent parts. The reference program is written for one: setup_inputs(seed, part) draws one part's arguments, and reference() takes and returns one part's arrays. A program takes and returns all parts, laid end to end along the dimension named above; an argument that names none is the same for every part.
All inputs are finite; a program needn't handle non-finite values.
Results may differ from the reference program's by a relative error of at most 0.018.
Values are sent between devices in bfloat16 or wider.
A program may use at most 768 MiB of HBM per device.

```python
import jax
import jax.numpy as jnp
from jax import lax

MICRO = 8
TOKENS = 512
D = 512
FF = 1280
LAYERS = 4
NAMES = ("w_gate", "w_up", "w_down")
SHAPES = {"w_gate": (LAYERS, D, FF), "w_up": (LAYERS, D, FF), "w_down": (LAYERS, FF, D)}


def bump(key, n, height):
    away = (jnp.arange(n, dtype=jnp.int32) - jax.random.randint(key, (), 0, n, jnp.int32)) % n
    return jnp.where(away < n // 8, height, 1.0)


def together(key, own, strength):
    shared = jax.random.normal(key, own.shape[1:], jnp.float32)
    return (own + strength * shared) * lax.rsqrt(1 + strength * strength)


def setup_inputs(seed: int = 0, part: int = 0) -> dict:
    kx, kdy, ka, kb, kz, kf, kh, kl, *kw = jax.random.split(jax.random.key(seed), 8 + len(NAMES))
    kx, kdy, ka, kb = (jax.random.fold_in(k, part) for k in (kx, kdy, ka, kb))
    shape = (MICRO, TOKENS, D)
    much_x, much_dy = jax.random.uniform(kz, (2,), jnp.float32, 0.0, 1.0)
    layers = 2.0 ** jax.random.uniform(kl, (LAYERS, 1, 1), jnp.float32, -1.0, 1.0)
    x = together(ka, jax.random.normal(kx, shape, jnp.float32), much_x) * bump(kf, D, 4.0)
    dy = together(kb, jax.random.normal(kdy, shape, jnp.float32), much_dy)
    drawn = {"x": x.astype(jnp.bfloat16), "dy": (dy * (MICRO * TOKENS) ** -0.5).astype(jnp.bfloat16)}
    for key, name in zip(kw, NAMES, strict=True):
        w = jax.random.normal(key, SHAPES[name], jnp.float32) * SHAPES[name][1] ** -0.5
        drawn[name] = (w * {"w_gate": 1.0, "w_up": bump(kh, FF, 4.0), "w_down": layers}[name]).astype(jnp.bfloat16)
    return drawn


def matmul(a, w):
    return jnp.dot(a, w, preferred_element_type=jnp.float32).astype(jnp.bfloat16)


def normed(h):
    wide = h.astype(jnp.float32)
    scale = lax.rsqrt(jnp.mean(wide**2, -1, keepdims=True) + 1e-6)
    return (wide * scale).astype(jnp.bfloat16)


def layer(h, w):
    a = normed(h)
    gate = jnp.dot(a, w["w_gate"], preferred_element_type=jnp.float32)
    up = jnp.dot(a, w["w_up"], preferred_element_type=jnp.float32)
    return h + matmul((jax.nn.silu(gate) * up).astype(jnp.bfloat16), w["w_down"])


def stack(weights, h):
    return lax.scan(lambda h, w: (layer(h, w), None), h, weights)[0]


def reference(x, dy, w_gate, w_up, w_down):
    weights = dict(zip(NAMES, (w_gate, w_up, w_down), strict=True))

    def take(so_far, one):
        h, by_y = one
        _, back = jax.vjp(lambda w: stack(w, h), weights)
        return jax.tree.map(lambda total, term: total + term.astype(jnp.float32), so_far, back(by_y)[0]), None

    none_yet = {name: jnp.zeros(w.shape, jnp.float32) for name, w in weights.items()}
    by_weights, _ = lax.scan(take, none_yet, (x, dy))
    return tuple(by_weights[name].astype(jnp.bfloat16) for name in NAMES)
```

```python
import functools

import jax
import jax.numpy as jnp
from jax import lax
from jax.experimental import pallas as pl
from jax.experimental.pallas import tpu as pltpu
from jax.sharding import PartitionSpec as P

MESH = pl.DeviceIdType.MESH
ROWS = 128
COLS = 256
LAG = 5
SENDS = 3
f32, bf16 = jnp.float32, jnp.bfloat16


def dot(a, b):
    return jnp.dot(a, b, preferred_element_type=f32)


def sigmoid(r):
    return 0.5 * jnp.tanh(0.5 * r) + 0.5


def kernel(stages, micro, tokens, x, dy, wg, wu, wd, out_g, out_u, out_d,
           fwd_in, bwd_in, fwd_out, bwd_out, g_ring, u_ring, act, dg, du, actc, a_t, dy_t,
           wg_v, wu_v, wd_v, wg_t, wu_t, wd_t, acc,
           fwd_sem, bwd_sem, fwd_send, bwd_send, w_sem, o_sem):
    me = lax.axis_index("pp")
    per = tokens // ROWS
    chunks = micro * per
    d, ff = wg_v.shape
    ring = g_ring.shape[0]
    first, last = me == 0, me == stages - 1
    lag = LAG * (stages - 1 - me)

    def load_x(i):
        return pltpu.make_async_copy(x.at[i // per, pl.ds(lax.rem(i, per) * ROWS, ROWS), :], fwd_in.at[i], fwd_sem.at[i])

    def load_dy(i):
        return pltpu.make_async_copy(dy.at[i // per, pl.ds(lax.rem(i, per) * ROWS, ROWS), :], bwd_in.at[i], bwd_sem.at[i])

    def onward(i):
        slot = lax.rem(i, SENDS)
        return pltpu.make_async_remote_copy(
            src_ref=fwd_out.at[slot], dst_ref=fwd_in.at[i], send_sem=fwd_send.at[slot], recv_sem=fwd_sem.at[i],
            device_id={"pp": me + 1}, device_id_type=MESH)

    def back(i):
        slot = lax.rem(i, SENDS)
        return pltpu.make_async_remote_copy(
            src_ref=bwd_out.at[slot], dst_ref=bwd_in.at[i], send_sem=bwd_send.at[slot], recv_sem=bwd_sem.at[i],
            device_id={"pp": me - 1}, device_id_type=MESH)

    loads = [pltpu.make_async_copy(src.at[0], dst, w_sem.at[n]) for n, (src, dst) in enumerate(((wg, wg_v), (wu, wu_v), (wd, wd_v)))]

    @pl.when(first)
    def _():
        load_x(0).start()
    for load in loads:
        load.start()

    @pl.when(first)
    def _():
        def go(i, c):
            load_x(i).start()
            return c
        lax.fori_loop(1, chunks, go, 0)

    @pl.when(last)
    def _():
        def go(i, c):
            load_dy(i).start()
            return c
        lax.fori_loop(0, chunks, go, 0)

    barrier = pltpu.get_barrier_semaphore()

    @pl.when(~first)
    def _():
        pl.semaphore_signal(barrier, inc=1, device_id={"pp": me - 1}, device_id_type=MESH)

    @pl.when(~last)
    def _():
        pl.semaphore_signal(barrier, inc=1, device_id={"pp": me + 1}, device_id_type=MESH)

    pl.semaphore_wait(barrier, jnp.where(first | last, 1, 2))

    for load in loads:
        load.wait()

    def turn(src, dst):
        def go(b, c):
            rows = pl.ds(pl.multiple_of(b * ROWS, ROWS), ROWS)
            dst[:, rows] = src[rows, :].T
            return c
        lax.fori_loop(0, src.shape[0] // ROWS, go, 0)

    @pl.when(~first)
    def _():
        turn(wd_v, wd_t)
        turn(wg_v, wg_t)
        turn(wu_v, wu_t)

    def norm(h):
        wide = h.astype(f32)
        scale = lax.rsqrt(jnp.sum(wide * wide, -1, keepdims=True) * (1.0 / d) + 1e-6)
        return wide, scale

    def forward(i):
        @pl.when(first)
        def _():
            load_x(i).wait()

        @pl.when(~first)
        def _():
            onward(i).wait_recv()
        slot = lax.rem(i, ring)
        h = fwd_in[i]
        wide, scale = norm(h)
        a = (wide * scale).astype(bf16)
        for t in range(0, ff, COLS):
            cols = slice(t, t + COLS)
            r = dot(a, wg_v[:, cols])
            s = dot(a, wu_v[:, cols])
            g_ring[slot, :, cols] = r
            u_ring[slot, :, cols] = s
            actc[:, cols] = (r * sigmoid(r) * s).astype(bf16)

        @pl.when(~last)
        def _():
            out = lax.rem(i, SENDS)
            y = dot(actc[...], wd_v[...]).astype(bf16)

            @pl.when(i >= SENDS)
            def _():
                onward(i - SENDS).wait_send()
            fwd_out[out] = (fwd_in[i].astype(f32) + y.astype(f32)).astype(bf16)
            onward(i).start()

    def backward(i):
        @pl.when(last)
        def _():
            load_dy(i).wait()

        @pl.when(~last)
        def _():
            back(i).wait_recv()
        slot, m, c = lax.rem(i, ring), lax.rem(i // per, 2), lax.rem(i, per)
        rows = pl.ds(pl.multiple_of(c * ROWS, ROWS), ROWS)
        by_y = bwd_in[i]
        wide, scale = norm(fwd_in[i])
        a_t[m, :, rows] = (wide * scale).astype(bf16).T
        dy_t[m, :, rows] = by_y.T
        for t in range(0, ff, COLS):
            cols = slice(t, t + COLS)
            by = dot(by_y, wd_t[:, cols]).astype(bf16).astype(f32)
            r, s = g_ring[slot, :, cols], u_ring[slot, :, cols]
            v = sigmoid(r)
            t_ = r * v
            act[m, rows, cols] = (t_ * s).astype(bf16)
            du[m, rows, cols] = (t_ * by).astype(bf16)
            bj = by * s
            dg[m, rows, cols] = (bj * v + (r * bj) * (v * (1.0 - v))).astype(bf16)

        @pl.when(~first)
        def _():
            out = lax.rem(i, SENDS)
            by_a = dot(du[m, rows, :], wu_t[...]).astype(bf16).astype(f32)
            by_a = (by_a + dot(dg[m, rows, :], wg_t[...]).astype(bf16).astype(f32)).astype(bf16).astype(f32)
            wide, scale = norm(fwd_in[i])
            along = jnp.sum(wide * by_a, -1, keepdims=True)
            by_h = (by_a * scale + (along * (scale * scale * scale * (-1.0 / d))) * wide).astype(bf16)

            @pl.when(i >= SENDS)
            def _():
                back(i - SENDS).wait_send()
            bwd_out[out] = (bwd_in[i].astype(f32) + by_h.astype(f32)).astype(bf16)
            back(i).start()

    outs = ((out_g, dg), (out_u, du), (out_d, act))

    def put(n, m, rows):
        hbm, stage = outs[n]
        return pltpu.make_async_copy(stage.at[m, rows, :], hbm.at[0, rows, :], o_sem.at[n])

    def weights(i):
        number, q = i // per, lax.rem(i, per)
        m = lax.rem(number, 2)
        rows = pl.ds(pl.multiple_of(q * ROWS, ROWS), ROWS)
        for n, (left, right) in enumerate(((a_t, dg), (a_t, du), (dy_t, act))):
            term = dot(left[m, rows, :], right[m]).astype(bf16).astype(f32)
            acc[n, rows, :] = jnp.where(number == 0, 0.0, acc[n, rows, :]) + term

        @pl.when(number == micro - 1)
        def _():
            for n in range(3):
                outs[n][1][1 - m, rows, :] = acc[n, rows, :].astype(bf16)
                put(n, 1 - m, rows).start()

    def step(i, carry):
        @pl.when(i < chunks)
        def _():
            forward(i)

        @pl.when(first & (i == 2))
        def _():
            turn(wd_v, wd_t)
        j = i - lag

        @pl.when((j >= 0) & (j < chunks))
        def _():
            backward(j)
        k = j - per

        @pl.when((k >= 0) & (k < chunks))
        def _():
            weights(k)
        return carry

    lax.fori_loop(0, chunks + LAG * (stages - 1) + per, step, 0)

    for n in range(SENDS):
        @pl.when(~last)
        def _():
            onward(chunks - SENDS + n).wait_send()

        @pl.when(~first)
        def _():
            back(chunks - SENDS + n).wait_send()
    m = (micro - 1) % 2
    for n in range(3):
        pltpu.make_async_copy(outs[n][1].at[1 - m], outs[n][0].at[0], o_sem.at[n]).wait()


def solution(mesh):
    stages = mesh.shape["pp"]

    def step(x, dy, wg, wu, wd):
        micro, tokens, d = x.shape
        ff = wg.shape[2]
        chunks = micro * (tokens // ROWS)
        ring = LAG * (stages - 1) + 1
        hbm = pl.BlockSpec(memory_space=pl.ANY)
        grad = jax.ShapeDtypeStruct((1, d, ff), bf16)
        g, u, down = pl.pallas_call(
            functools.partial(kernel, stages, micro, tokens),
            out_shape=(grad, grad, grad),
            in_specs=[hbm] * 5,
            out_specs=(hbm,) * 3,
            scratch_shapes=[
                pltpu.VMEM((chunks, ROWS, d), bf16),
                pltpu.VMEM((chunks, ROWS, d), bf16),
                pltpu.VMEM((SENDS, ROWS, d), bf16),
                pltpu.VMEM((SENDS, ROWS, d), bf16),
                pltpu.VMEM((ring, ROWS, ff), f32),
                pltpu.VMEM((ring, ROWS, ff), f32),
                pltpu.VMEM((2, tokens, ff), bf16),
                pltpu.VMEM((2, tokens, ff), bf16),
                pltpu.VMEM((2, tokens, ff), bf16),
                pltpu.VMEM((ROWS, ff), bf16),
                pltpu.VMEM((2, d, tokens), bf16),
                pltpu.VMEM((2, d, tokens), bf16),
                pltpu.VMEM((d, ff), bf16),
                pltpu.VMEM((d, ff), bf16),
                pltpu.VMEM((ff, d), bf16),
                pltpu.VMEM((ff, d), bf16),
                pltpu.VMEM((ff, d), bf16),
                pltpu.VMEM((d, ff), bf16),
                pltpu.VMEM((3, d, ff), f32),
                pltpu.SemaphoreType.DMA((chunks,)),
                pltpu.SemaphoreType.DMA((chunks,)),
                pltpu.SemaphoreType.DMA((SENDS,)),
                pltpu.SemaphoreType.DMA((SENDS,)),
                pltpu.SemaphoreType.DMA((3,)),
                pltpu.SemaphoreType.DMA((3,)),
            ],
            compiler_params=pltpu.CompilerParams(collective_id=0, has_side_effects=True, vmem_limit_bytes=67_043_328),
        )(x, dy, wg, wu, wd)
        return g, u, down.swapaxes(1, 2)

    return jax.shard_map(
        step,
        mesh=mesh,
        in_specs=(P("rep", None, None),) * 2 + (P("pp", None, None),) * 3,
        out_specs=(P(("rep", "pp"), None, None),) * 3,
        check_vma=False,
    )
```

```python
import functools

import jax
import jax.numpy as jnp
from jax import lax
from jax.experimental import pallas as pl
from jax.experimental.pallas import tpu as pltpu
from jax.sharding import PartitionSpec as P

MESH = pl.DeviceIdType.MESH
ROWS = 128
COLS = 256
LAGS = (13,8,4,0)
SENDS = 3
f32, bf16 = jnp.float32, jnp.bfloat16


def dot(a, b):
    return jnp.dot(a, b, preferred_element_type=f32)


def chunk(c):
    return pl.ds(pl.multiple_of(c * ROWS, ROWS), ROWS)


def kernel(stages, micro, tokens, x, dy, wg, wu, wd,
           acc, act, a_t, dg, du, dy_t,
           fwd_in, bwd_in, fwd_out, bwd_out, t_ring, q_ring,
           wg_v, wu_v, wd_v, wg_t, wu_t, wd_t,
           fwd_sem, bwd_sem, fwd_send, bwd_send, w_sem):
    me = lax.axis_index("pp")
    per = tokens // ROWS
    chunks = micro * per
    d, ff = wg_v.shape
    ring, held = t_ring.shape[0], act.shape[0]
    first, last = me == 0, me == stages - 1
    lag = sum(jnp.where(me == n, by, 0) for n, by in enumerate(LAGS))

    def load_x(i):
        return pltpu.make_async_copy(x.at[i // per, chunk(lax.rem(i, per)), :], fwd_in.at[i], fwd_sem.at[i])

    def load_dy(i):
        return pltpu.make_async_copy(dy.at[i // per, chunk(lax.rem(i, per)), :], bwd_in.at[i], bwd_sem.at[i])

    def onward(i):
        slot = lax.rem(i, SENDS)
        return pltpu.make_async_remote_copy(
            src_ref=fwd_out.at[slot], dst_ref=fwd_in.at[i], send_sem=fwd_send.at[slot], recv_sem=fwd_sem.at[i],
            device_id={"pp": me + 1}, device_id_type=MESH)

    def back(i):
        slot = lax.rem(i, SENDS)
        return pltpu.make_async_remote_copy(
            src_ref=bwd_out.at[slot], dst_ref=bwd_in.at[i], send_sem=bwd_send.at[slot], recv_sem=bwd_sem.at[i],
            device_id={"pp": me - 1}, device_id_type=MESH)

    loads = [pltpu.make_async_copy(src.at[0], dst, w_sem.at[n]) for n, (src, dst) in enumerate(((wg, wg_v), (wu, wu_v), (wd, wd_v)))]

    @pl.when(first)
    def _():
        load_x(0).start()
    for load in loads:
        load.start()

    @pl.when(first)
    def _():
        def go(i, c):
            load_x(i).start()
            return c
        lax.fori_loop(1, chunks, go, 0)

    @pl.when(last)
    def _():
        def go(i, c):
            load_dy(i).start()
            return c
        lax.fori_loop(0, chunks, go, 0)

    barrier = pltpu.get_barrier_semaphore()

    @pl.when(~first)
    def _():
        pl.semaphore_signal(barrier, inc=1, device_id={"pp": me - 1}, device_id_type=MESH)

    @pl.when(~last)
    def _():
        pl.semaphore_signal(barrier, inc=1, device_id={"pp": me + 1}, device_id_type=MESH)

    pl.semaphore_wait(barrier, jnp.where(first | last, 1, 2))

    for load in loads:
        load.wait()

    def turn(src, dst):
        def go(b, c):
            dst[:, chunk(b)] = src[chunk(b), :].T
            return c
        lax.fori_loop(0, src.shape[0] // ROWS, go, 0)

    @pl.when(~first)
    def _():
        turn(wd_v, wd_t)
        turn(wg_v, wg_t)
        turn(wu_v, wu_t)

    def norm(h):
        wide = h.astype(f32)
        scale = lax.rsqrt(jnp.sum(wide * wide, -1, keepdims=True) * (1.0 / d) + 1e-6)
        return wide, scale

    def forward_wait(i):
        @pl.when(first)
        def _():
            load_x(i).wait()

        @pl.when(~first)
        def _():
            onward(i).wait_recv()

        @pl.when(~last & (i >= SENDS))
        def _():
            onward(i - SENDS).wait_send()

    def gate_up(i):
        slot, m, rows = lax.rem(i, ring), lax.rem(i // per, held), chunk(lax.rem(i, per))
        wide, scale = norm(fwd_in[i])
        a = (wide * scale).astype(bf16)
        a_t[m, :, rows] = a.T
        for t in range(0, ff, COLS):
            cols = slice(t, t + COLS)
            r, s = dot(a, wg_v[:, cols]), dot(a, wu_v[:, cols])
            v = 0.5 * jnp.tanh(0.5 * r) + 0.5
            silu = r * v
            t_ring[slot, :, cols] = silu
            q_ring[slot, :, cols] = s * (v + silu * (1.0 - v))
            act[m, rows, cols] = (silu * s).astype(bf16)

    def down(i):
        m, rows = lax.rem(i // per, held), chunk(lax.rem(i, per))
        y = dot(act[m, rows, :], wd_v[...]).astype(bf16)
        fwd_out[lax.rem(i, SENDS)] = (fwd_in[i].astype(f32) + y.astype(f32)).astype(bf16)

    def forward_send(i):
        @pl.when(~last)
        def _():
            onward(i).start()

    def backward_wait(i):
        @pl.when(last)
        def _():
            load_dy(i).wait()

        @pl.when(~last)
        def _():
            back(i).wait_recv()

        @pl.when(~first & (i >= SENDS))
        def _():
            back(i - SENDS).wait_send()

    def by_gate_up(i):
        slot, m, rows = lax.rem(i, ring), lax.rem(i // per, 2), chunk(lax.rem(i, per))
        by_y = bwd_in[i]
        dy_t[m, :, rows] = by_y.T
        for t in range(0, ff, COLS):
            cols = slice(t, t + COLS)
            by = dot(by_y, wd_t[:, cols]).astype(bf16).astype(f32)
            du[m, rows, cols] = (t_ring[slot, :, cols] * by).astype(bf16)
            dg[m, rows, cols] = (q_ring[slot, :, cols] * by).astype(bf16)

    def by_input(i):
        m, rows = lax.rem(i // per, 2), chunk(lax.rem(i, per))
        by_a = dot(du[m, rows, :], wu_t[...]).astype(bf16).astype(f32)
        by_a = (by_a + dot(dg[m, rows, :], wg_t[...]).astype(bf16).astype(f32)).astype(bf16).astype(f32)
        wide, scale = norm(fwd_in[i])
        along = jnp.sum(wide * by_a, -1, keepdims=True)
        by_h = (by_a * scale + (along * (scale * scale * scale * (-1.0 / d))) * wide).astype(bf16)
        bwd_out[lax.rem(i, SENDS)] = (bwd_in[i].astype(f32) + by_h.astype(f32)).astype(bf16)

    def backward_send(i):
        @pl.when(~first)
        def _():
            back(i).start()

    def weights(i):
        number, rows = i // per, chunk(lax.rem(i, per))
        m, w = lax.rem(number, 2), lax.rem(number, held)
        for n, (left, right) in enumerate(((a_t.at[w], dg.at[m]), (a_t.at[w], du.at[m]), (dy_t.at[m], act.at[w]))):
            term = dot(left[rows, :], right[...]).astype(bf16).astype(f32)
            acc[n, rows, :] = jnp.where(number == 0, 0.0, acc[n, rows, :]) + term

    def step(i, carry):
        j = i - lag
        k = j - per
        forth, backwards, heavy = i < chunks, (j >= 0) & (j < chunks), (k >= 0) & (k < chunks - per)

        @pl.when(forth)
        def _():
            forward_wait(i)
            gate_up(i)

            @pl.when(~last)
            def _():
                down(i)
            forward_send(i)

        @pl.when(first & (i == 2))
        def _():
            turn(wd_v, wd_t)

        @pl.when(backwards)
        def _():
            backward_wait(j)
            by_gate_up(j)

            @pl.when(~first)
            def _():
                by_input(j)
            backward_send(j)

        @pl.when(heavy)
        def _():
            weights(k)
        return carry

    lax.fori_loop(0, chunks + max(LAGS), step, 0)

    for n in range(SENDS):
        @pl.when(~last)
        def _():
            onward(chunks - SENDS + n).wait_send()

        @pl.when(~first)
        def _():
            back(chunks - SENDS + n).wait_send()


def finish(w, m, acc, act, a_t, dg, du, dy_t, out_g, out_u, out_d, stage, turned, sem):
    d = acc.shape[1]
    copies = []
    for n, (left, right, out) in enumerate(((dy_t.at[m], act.at[w], out_d), (a_t.at[w], dg.at[m], out_g), (a_t.at[w], du.at[m], out_u))):
        for q in range(0, d, ROWS):
            rows = slice(q, q + ROWS)
            term = dot(left[rows, :], right[...]).astype(bf16).astype(f32)
            total = (acc[(n + 2) % 3, rows, :] + term).astype(bf16)
            if n == 0:
                turned[:, rows] = total.T
                copy = pltpu.make_async_copy(turned.at[:, rows], out.at[0, :, rows], sem.at[n, q // ROWS])
            else:
                stage[n - 1, rows, :] = total
                copy = pltpu.make_async_copy(stage.at[n - 1, rows, :], out.at[0, rows, :], sem.at[n, q // ROWS])
            copy.start()
            copies.append(copy)
    for copy in copies:
        copy.wait()


def solution(mesh):
    stages = mesh.shape["pp"]

    def step(x, dy, wg, wu, wd):
        micro, tokens, d = x.shape
        ff = wg.shape[2]
        per = tokens // ROWS
        chunks = micro * per
        ring = max(LAGS) + 1
        held = pl.cdiv(ring - 1 + per, per) + 1
        hbm, vmem = pl.BlockSpec(memory_space=pl.ANY), pl.BlockSpec(memory_space=pltpu.VMEM)
        sums = pl.pallas_call(
            functools.partial(kernel, stages, micro, tokens),
            out_shape=(
                pltpu.VMEM((3, d, ff), f32),
                pltpu.VMEM((held, tokens, ff), bf16),
                pltpu.VMEM((held, d, tokens), bf16),
                pltpu.VMEM((2, tokens, ff), bf16),
                pltpu.VMEM((2, tokens, ff), bf16),
                pltpu.VMEM((2, d, tokens), bf16),
            ),
            in_specs=[hbm] * 5,
            out_specs=(vmem,) * 6,
            scratch_shapes=[
                pltpu.VMEM((chunks, ROWS, d), bf16),
                pltpu.VMEM((chunks, ROWS, d), bf16),
                pltpu.VMEM((SENDS, ROWS, d), bf16),
                pltpu.VMEM((SENDS, ROWS, d), bf16),
                pltpu.VMEM((ring, ROWS, ff), f32),
                pltpu.VMEM((ring, ROWS, ff), f32),
                pltpu.VMEM((d, ff), bf16),
                pltpu.VMEM((d, ff), bf16),
                pltpu.VMEM((ff, d), bf16),
                pltpu.VMEM((ff, d), bf16),
                pltpu.VMEM((ff, d), bf16),
                pltpu.VMEM((d, ff), bf16),
                pltpu.SemaphoreType.DMA((chunks,)),
                pltpu.SemaphoreType.DMA((chunks,)),
                pltpu.SemaphoreType.DMA((SENDS,)),
                pltpu.SemaphoreType.DMA((SENDS,)),
                pltpu.SemaphoreType.DMA((3,)),
            ],
            compiler_params=pltpu.CompilerParams(collective_id=0, has_side_effects=True, vmem_limit_bytes=38 * 2**20),
        )(x, dy, wg, wu, wd)
        return pl.pallas_call(
            functools.partial(finish, (micro - 1) % held, (micro - 1) % 2),
            out_shape=(
                jax.ShapeDtypeStruct((1, d, ff), bf16),
                jax.ShapeDtypeStruct((1, d, ff), bf16),
                jax.ShapeDtypeStruct((1, ff, d), bf16),
            ),
            in_specs=[vmem] * 6,
            out_specs=(hbm,) * 3,
            scratch_shapes=[pltpu.VMEM((2, d, ff), bf16), pltpu.VMEM((ff, d), bf16), pltpu.SemaphoreType.DMA((3, d // ROWS))],
            compiler_params=pltpu.CompilerParams(has_side_effects=True, vmem_limit_bytes=8 * 2**20),
        )(*sums)

    return jax.shard_map(
        step,
        mesh=mesh,
        in_specs=(P("rep", None, None),) * 2 + (P("pp", None, None),) * 3,
        out_specs=(P(("rep", "pp"), None, None),) * 3,
        check_vma=False,
    )
```

```python
import functools

import jax
import jax.numpy as jnp
from jax import lax
from jax.experimental import pallas as pl
from jax.experimental.pallas import tpu as pltpu
from jax.sharding import PartitionSpec as P

MESH = pl.DeviceIdType.MESH
ROWS = 128
COLS = 256
LAGS = (13,8,4,0)
SENDS = 3
f32, bf16 = jnp.float32, jnp.bfloat16


def dot(a, b):
    return jnp.dot(a, b, preferred_element_type=f32)


def chunk(c):
    return pl.ds(pl.multiple_of(c * ROWS, ROWS), ROWS)


def tiles(a_t, dy_t, dg, du, act):
    for n, left, right in ((2, dy_t, act), (0, a_t, dg), (1, a_t, du)):
        for t in range(0, right.shape[1], COLS):
            yield n, slice(t, t + COLS), left, right


def kernel(stages, micro, tokens, x, dy, wg, wu, wd,
           acc, act_out, a_out, dg, du, dy_t, t_ring,
           fwd_in, bwd_in, fwd_out, bwd_out, q_ring, by_act, act, a_t,
           wg_v, wu_v, wd_v, wg_t, wu_t, wd_t,
           fwd_sem, bwd_sem, fwd_send, bwd_send, w_sem):
    me = lax.axis_index("pp")
    per = tokens // ROWS
    chunks = micro * per
    d, ff = wg_v.shape
    ring, held = t_ring.shape[0], act.shape[0]
    first, last = me == 0, me == stages - 1
    lag = sum(jnp.where(me == n, by, 0) for n, by in enumerate(LAGS))

    def load_x(i):
        return pltpu.make_async_copy(x.at[i // per, chunk(lax.rem(i, per)), :], fwd_in.at[i], fwd_sem.at[i])

    def load_dy(i):
        return pltpu.make_async_copy(dy.at[i // per, chunk(lax.rem(i, per)), :], bwd_in.at[i], bwd_sem.at[i])

    def onward(i):
        slot = lax.rem(i, SENDS)
        return pltpu.make_async_remote_copy(
            src_ref=fwd_out.at[slot], dst_ref=fwd_in.at[i], send_sem=fwd_send.at[slot], recv_sem=fwd_sem.at[i],
            device_id={"pp": me + 1}, device_id_type=MESH)

    def back(i):
        slot = lax.rem(i, SENDS)
        return pltpu.make_async_remote_copy(
            src_ref=bwd_out.at[slot], dst_ref=bwd_in.at[i], send_sem=bwd_send.at[slot], recv_sem=bwd_sem.at[i],
            device_id={"pp": me - 1}, device_id_type=MESH)

    loads = [pltpu.make_async_copy(src.at[0], dst, w_sem.at[n]) for n, (src, dst) in enumerate(((wg, wg_v), (wu, wu_v), (wd, wd_v)))]

    @pl.when(first)
    def _():
        load_x(0).start()
    for load in loads:
        load.start()

    @pl.when(first)
    def _():
        def go(i, c):
            load_x(i).start()
            return c
        lax.fori_loop(1, chunks, go, 0)

    @pl.when(last)
    def _():
        def go(i, c):
            load_dy(i).start()
            return c
        lax.fori_loop(0, chunks, go, 0)

    barrier = pltpu.get_barrier_semaphore()

    @pl.when(~first)
    def _():
        pl.semaphore_signal(barrier, inc=1, device_id={"pp": me - 1}, device_id_type=MESH)

    @pl.when(~last)
    def _():
        pl.semaphore_signal(barrier, inc=1, device_id={"pp": me + 1}, device_id_type=MESH)

    pl.semaphore_wait(barrier, jnp.where(first | last, 1, 2))

    for load in loads:
        load.wait()

    def turn(src, dst):
        def go(b, c):
            dst[:, chunk(b)] = src[chunk(b), :].T
            return c
        lax.fori_loop(0, src.shape[0] // ROWS, go, 0)

    @pl.when(~first)
    def _():
        turn(wd_v, wd_t)
        turn(wg_v, wg_t)
        turn(wu_v, wu_t)

    def norm(h):
        wide = h.astype(f32)
        scale = lax.rsqrt(jnp.sum(wide * wide, -1, keepdims=True) * (1.0 / d) + 1e-6)
        return wide, scale

    def forward_wait(i):
        @pl.when(first)
        def _():
            load_x(i).wait()

        @pl.when(~first)
        def _():
            onward(i).wait_recv()

        @pl.when(i >= SENDS)
        def _():
            onward(i - SENDS).wait_send()

    def gate_up(i, by_ref=None):
        slot, m, rows = lax.rem(i, ring), lax.rem(i // per, held), chunk(lax.rem(i, per))
        wide, scale = norm(fwd_in[i])
        a = (wide * scale).astype(bf16)
        a_t[m, :, rows] = a.T
        for t in range(0, ff, COLS):
            cols = slice(t, t + COLS)
            r, s = dot(a, wg_v[:, cols]), dot(a, wu_v[:, cols])
            v = 0.5 * jnp.tanh(0.5 * r) + 0.5
            silu = r * v
            slope = s * (v + silu * (1.0 - v))
            act[m, rows, cols] = (silu * s).astype(bf16)
            if by_ref is None:
                t_ring[slot, :, cols] = silu
                q_ring[slot, :, cols] = slope
            else:
                by = by_ref[:, cols].astype(f32)
                b = lax.rem(i // per, 2)
                du[b, rows, cols] = (silu * by).astype(bf16)
                dg[b, rows, cols] = (slope * by).astype(bf16)

    def down(i):
        m, rows = lax.rem(i // per, held), chunk(lax.rem(i, per))
        y = dot(act[m, rows, :], wd_v[...]).astype(bf16)
        fwd_out[lax.rem(i, SENDS)] = (fwd_in[i].astype(f32) + y.astype(f32)).astype(bf16)

    def by_hidden(i):
        load_dy(i).wait()
        by_y = bwd_in[i]
        dy_t[lax.rem(i // per, 2), :, chunk(lax.rem(i, per))] = by_y.T
        by_act[...] = dot(by_y, wd_t[...]).astype(bf16)

    def by_gate_up(i):
        slot, m, rows = lax.rem(i, ring), lax.rem(i // per, 2), chunk(lax.rem(i, per))
        by_y = bwd_in[i]
        dy_t[m, :, rows] = by_y.T
        for t in range(0, ff, COLS):
            cols = slice(t, t + COLS)
            by = dot(by_y, wd_t[:, cols]).astype(bf16).astype(f32)
            du[m, rows, cols] = (t_ring[slot, :, cols] * by).astype(bf16)
            dg[m, rows, cols] = (q_ring[slot, :, cols] * by).astype(bf16)

    def by_input(i):
        m, rows = lax.rem(i // per, 2), chunk(lax.rem(i, per))
        by_a = dot(du[m, rows, :], wu_t[...]).astype(bf16).astype(f32)
        by_a = (by_a + dot(dg[m, rows, :], wg_t[...]).astype(bf16).astype(f32)).astype(bf16).astype(f32)
        wide, scale = norm(fwd_in[i])
        along = jnp.sum(wide * by_a, -1, keepdims=True)
        by_h = (by_a * scale + (along * (scale * scale * scale * (-1.0 / d))) * wide).astype(bf16)
        bwd_out[lax.rem(i, SENDS)] = (bwd_in[i].astype(f32) + by_h.astype(f32)).astype(bf16)

    def weights(i):
        number, rows = i // per, chunk(lax.rem(i, per))
        m, w = lax.rem(number, 2), lax.rem(number, held)
        for n, (left, right) in enumerate(((a_t.at[w], dg.at[m]), (a_t.at[w], du.at[m]), (dy_t.at[m], act.at[w]))):
            term = dot(left[rows, :], right[...]).astype(bf16).astype(f32)
            acc[n, rows, :] = jnp.where(number == 0, 0.0, acc[n, rows, :]) + term

    def half():
        m, w, mid = (micro - 1) % 2, (micro - 1) % held, tokens // 2
        for n, cols, left, right in tiles(a_t.at[w], dy_t.at[m], dg.at[m], du.at[m], act.at[w]):
            term = dot(left[:, :mid], right[:mid, cols])
            for q in range(d // ROWS):
                t_ring[(chunks + n * (d // ROWS) + q) % ring, :, cols] = term[q * ROWS:(q + 1) * ROWS]
        act_out[...] = act[w, mid:, :]
        a_out[...] = a_t[w, :, mid:]

    def step(i, carry):
        j = i - lag
        k = j - per
        forth, backwards = i < chunks, (j >= 0) & (j < chunks)

        @pl.when(last & forth)
        def _():
            onward(i).wait_recv()

            @pl.when(i >= SENDS)
            def _():
                back(i - SENDS).wait_send()
            gate_up(i, by_act)
            by_input(i)
            back(i).start()

        @pl.when(~last & forth)
        def _():
            forward_wait(i)
            gate_up(i)
            down(i)
            onward(i).start()

        @pl.when(first & (i == 2))
        def _():
            turn(wd_v, wd_t)

        @pl.when(~last & backwards)
        def _():
            back(j).wait_recv()

            @pl.when(~first & (j >= SENDS))
            def _():
                back(j - SENDS).wait_send()

            @pl.when(first)
            def _():
                by_gate_up(j)

            @pl.when(~first)
            def _():
                by_gate_up(j)
                by_input(j)
                back(j).start()

        hurry = first & (j >= chunks - per)
        low = jnp.where(hurry, chunks - 2 * per + 2 * (j - chunks + per), jnp.maximum(k, 0))
        high = jnp.minimum(jnp.where(hurry, low + 2, k + 1), chunks - per)

        def share(n, c):
            weights(n)
            return c
        lax.fori_loop(low, high, share, 0)

        @pl.when(last & (i < chunks - 1))
        def _():
            by_hidden(i + 1)

        @pl.when(j == jnp.where(first, chunks - 2, chunks - 1))
        def _():
            half()
        return carry

    @pl.when(last)
    def _():
        by_hidden(0)

    lax.fori_loop(0, chunks + max(LAGS), step, 0)

    for n in range(SENDS):
        @pl.when(~last)
        def _():
            onward(chunks - SENDS + n).wait_send()

        @pl.when(~first)
        def _():
            back(chunks - SENDS + n).wait_send()


def finish(m, chunks, acc, act, a_t, dg, du, dy_t, t_ring, out_g, out_u, out_d, stage, turned, sem):
    d, mid = acc.shape[1], act.shape[0]
    copies = []
    for p, (n, cols, left, right) in enumerate(tiles(a_t, dy_t.at[m, :, mid:], dg.at[m, mid:, :], du.at[m, mid:, :], act)):
        second = dot(left[...], right[:, cols])
        for q in range(d // ROWS):
            rows = slice(q * ROWS, (q + 1) * ROWS)
            term = t_ring[(chunks + n * (d // ROWS) + q) % t_ring.shape[0], :, cols] + second[rows]
            total = (acc[n, rows, cols] + term.astype(bf16).astype(f32)).astype(bf16)
            if n == 2:
                turned[cols, rows] = total.T
            else:
                stage[n, rows, cols] = total
        if n == 2:
            copy = pltpu.make_async_copy(turned.at[cols, :], out_d.at[0, cols, :], sem.at[p])
        else:
            copy = pltpu.make_async_copy(stage.at[n, :, cols], (out_g, out_u)[n].at[0, :, cols], sem.at[p])
        copy.start()
        copies.append(copy)
    for copy in copies:
        copy.wait()


def solution(mesh):
    stages = mesh.shape["pp"]

    def step(x, dy, wg, wu, wd):
        micro, tokens, d = x.shape
        ff = wg.shape[2]
        per = tokens // ROWS
        chunks = micro * per
        ring = max(LAGS) + 1
        held = pl.cdiv(ring - 1 + per, per) + 1
        hbm, vmem = pl.BlockSpec(memory_space=pl.ANY), pl.BlockSpec(memory_space=pltpu.VMEM)
        sums = pl.pallas_call(
            functools.partial(kernel, stages, micro, tokens),
            out_shape=(
                pltpu.VMEM((3, d, ff), f32),
                pltpu.VMEM((tokens // 2, ff), bf16),
                pltpu.VMEM((d, tokens // 2), bf16),
                pltpu.VMEM((2, tokens, ff), bf16),
                pltpu.VMEM((2, tokens, ff), bf16),
                pltpu.VMEM((2, d, tokens), bf16),
                pltpu.VMEM((ring, ROWS, ff), f32),
            ),
            in_specs=[hbm] * 5,
            out_specs=(vmem,) * 7,
            scratch_shapes=[
                pltpu.VMEM((chunks, ROWS, d), bf16),
                pltpu.VMEM((chunks, ROWS, d), bf16),
                pltpu.VMEM((SENDS, ROWS, d), bf16),
                pltpu.VMEM((SENDS, ROWS, d), bf16),
                pltpu.VMEM((ring, ROWS, ff), f32),
                pltpu.VMEM((ROWS, ff), bf16),
                pltpu.VMEM((held, tokens, ff), bf16),
                pltpu.VMEM((held, d, tokens), bf16),
                pltpu.VMEM((d, ff), bf16),
                pltpu.VMEM((d, ff), bf16),
                pltpu.VMEM((ff, d), bf16),
                pltpu.VMEM((ff, d), bf16),
                pltpu.VMEM((ff, d), bf16),
                pltpu.VMEM((d, ff), bf16),
                pltpu.SemaphoreType.DMA((chunks,)),
                pltpu.SemaphoreType.DMA((chunks,)),
                pltpu.SemaphoreType.DMA((SENDS,)),
                pltpu.SemaphoreType.DMA((SENDS,)),
                pltpu.SemaphoreType.DMA((3,)),
            ],
            compiler_params=pltpu.CompilerParams(collective_id=0, has_side_effects=True, vmem_limit_bytes=39 * 2**20),
        )(x, dy, wg, wu, wd)
        return pl.pallas_call(
            functools.partial(finish, (micro - 1) % 2, chunks),
            out_shape=(
                jax.ShapeDtypeStruct((1, d, ff), bf16),
                jax.ShapeDtypeStruct((1, d, ff), bf16),
                jax.ShapeDtypeStruct((1, ff, d), bf16),
            ),
            in_specs=[vmem] * 7,
            out_specs=(hbm,) * 3,
            scratch_shapes=[pltpu.VMEM((2, d, ff), bf16), pltpu.VMEM((ff, d), bf16), pltpu.SemaphoreType.DMA((3 * (ff // COLS),))],
            compiler_params=pltpu.CompilerParams(has_side_effects=True, vmem_limit_bytes=8 * 2**20),
        )(*sums)

    return jax.shard_map(
        step,
        mesh=mesh,
        in_specs=(P("rep", None, None),) * 2 + (P("pp", None, None),) * 3,
        out_specs=(P(("rep", "pp"), None, None),) * 3,
        check_vma=False,
    )
```

```python
import functools

import jax
import jax.numpy as jnp
from jax import lax
from jax.experimental import pallas as pl
from jax.experimental.pallas import tpu as pltpu
from jax.sharding import PartitionSpec as P

MESH = pl.DeviceIdType.MESH
ROWS = 128
COLS = 256
LAGS = (13,8,4,0)
STAGGER = 800
SENDS = 3
f32, bf16 = jnp.float32, jnp.bfloat16


def dot(a, b):
    return jnp.dot(a, b, preferred_element_type=f32)


def chunk(c):
    return pl.ds(pl.multiple_of(c * ROWS, ROWS), ROWS)


def tiles(a_t, dy_t, dg, du, act):
    for n, left, right in ((2, dy_t, act), (0, a_t, dg), (1, a_t, du)):
        for t in range(0, right.shape[1], COLS):
            yield n, slice(t, t + COLS), left, right


def kernel(stages, micro, tokens, x, dy, wg, wu, wd,
           acc, act_out, a_out, dg, du, dy_t, t_ring,
           fwd_in, bwd_in, fwd_out, bwd_out, q_ring, by_act, act, a_t,
           wg_v, wu_v, wd_v, wg_t, wu_t, wd_t,
           fwd_sem, bwd_sem, fwd_send, bwd_send, w_sem):
    me = lax.axis_index("pp")
    per = tokens // ROWS
    chunks = micro * per
    d, ff = wg_v.shape
    ring, held = t_ring.shape[0], act.shape[0]
    first, last = me == 0, me == stages - 1
    lag = sum(jnp.where(me == n, by, 0) for n, by in enumerate(LAGS))

    def load_x(i):
        return pltpu.make_async_copy(x.at[i // per, chunk(lax.rem(i, per)), :], fwd_in.at[i], fwd_sem.at[i])

    def load_dy(i):
        return pltpu.make_async_copy(dy.at[i // per, chunk(lax.rem(i, per)), :], bwd_in.at[i], bwd_sem.at[i])

    def onward(i):
        slot = lax.rem(i, SENDS)
        return pltpu.make_async_remote_copy(
            src_ref=fwd_out.at[slot], dst_ref=fwd_in.at[i], send_sem=fwd_send.at[slot], recv_sem=fwd_sem.at[i],
            device_id={"pp": me + 1}, device_id_type=MESH)

    def back(i):
        slot = lax.rem(i, SENDS)
        return pltpu.make_async_remote_copy(
            src_ref=bwd_out.at[slot], dst_ref=bwd_in.at[i], send_sem=bwd_send.at[slot], recv_sem=bwd_sem.at[i],
            device_id={"pp": me - 1}, device_id_type=MESH)

    loads = [pltpu.make_async_copy(src.at[0], dst, w_sem.at[n]) for n, (src, dst) in enumerate(((wg, wg_v), (wu, wu_v), (wd, wd_v)))]

    @pl.when(first)
    def _():
        load_x(0).start()
    for load in loads:
        load.start()

    @pl.when(first)
    def _():
        def go(i, c):
            load_x(i).start()
            return c
        lax.fori_loop(1, chunks, go, 0)

    @pl.when(last)
    def _():
        def go(i, c):
            load_dy(i).start()
            return c
        lax.fori_loop(0, chunks, go, 0)

    barrier = pltpu.get_barrier_semaphore()

    @pl.when(~first)
    def _():
        pl.semaphore_signal(barrier, inc=1, device_id={"pp": me - 1}, device_id_type=MESH)

    @pl.when(~last)
    def _():
        pl.semaphore_signal(barrier, inc=1, device_id={"pp": me + 1}, device_id_type=MESH)

    pl.semaphore_wait(barrier, jnp.where(first | last, 1, 2))

    for load in loads:
        load.wait()

    def turn(src, dst):
        def go(b, c):
            dst[:, chunk(b)] = src[chunk(b), :].T
            return c
        lax.fori_loop(0, src.shape[0] // ROWS, go, 0)

    @pl.when(~first)
    def _():
        turn(wd_v, wd_t)
        turn(wg_v, wg_t)
        turn(wu_v, wu_t)

    def norm(h):
        wide = h.astype(f32)
        scale = lax.rsqrt(jnp.sum(wide * wide, -1, keepdims=True) * (1.0 / d) + 1e-6)
        return wide, scale

    def forward_wait(i):
        @pl.when(first)
        def _():
            load_x(i).wait()

        @pl.when(~first)
        def _():
            onward(i).wait_recv()

        @pl.when(i >= SENDS)
        def _():
            onward(i - SENDS).wait_send()

    def gate_up(i, by_ref=None):
        slot, m, rows = lax.rem(i, ring), lax.rem(i // per, held), chunk(lax.rem(i, per))
        wide, scale = norm(fwd_in[i])
        a = (wide * scale).astype(bf16)
        a_t[m, :, rows] = a.T
        for t in range(0, ff, COLS):
            cols = slice(t, t + COLS)
            r, s = dot(a, wg_v[:, cols]), dot(a, wu_v[:, cols])
            v = 0.5 * jnp.tanh(0.5 * r) + 0.5
            silu = r * v
            slope = s * (v + silu * (1.0 - v))
            act[m, rows, cols] = (silu * s).astype(bf16)
            if by_ref is None:
                t_ring[slot, :, cols] = silu
                q_ring[slot, :, cols] = slope
            else:
                by = by_ref[:, cols].astype(f32)
                b = lax.rem(i // per, 2)
                du[b, rows, cols] = (silu * by).astype(bf16)
                dg[b, rows, cols] = (slope * by).astype(bf16)

    def down(i):
        m, rows = lax.rem(i // per, held), chunk(lax.rem(i, per))
        y = dot(act[m, rows, :], wd_v[...]).astype(bf16)
        fwd_out[lax.rem(i, SENDS)] = (fwd_in[i].astype(f32) + y.astype(f32)).astype(bf16)

    def by_hidden(i):
        load_dy(i).wait()
        by_y = bwd_in[i]
        dy_t[lax.rem(i // per, 2), :, chunk(lax.rem(i, per))] = by_y.T
        by_act[...] = dot(by_y, wd_t[...]).astype(bf16)

    def by_gate_up(i):
        slot, m, rows = lax.rem(i, ring), lax.rem(i // per, 2), chunk(lax.rem(i, per))
        by_y = bwd_in[i]
        dy_t[m, :, rows] = by_y.T
        for t in range(0, ff, COLS):
            cols = slice(t, t + COLS)
            by = dot(by_y, wd_t[:, cols]).astype(bf16).astype(f32)
            du[m, rows, cols] = (t_ring[slot, :, cols] * by).astype(bf16)
            dg[m, rows, cols] = (q_ring[slot, :, cols] * by).astype(bf16)

    def by_input(i):
        m, rows = lax.rem(i // per, 2), chunk(lax.rem(i, per))
        by_a = dot(du[m, rows, :], wu_t[...]).astype(bf16).astype(f32)
        by_a = (by_a + dot(dg[m, rows, :], wg_t[...]).astype(bf16).astype(f32)).astype(bf16).astype(f32)
        wide, scale = norm(fwd_in[i])
        along = jnp.sum(wide * by_a, -1, keepdims=True)
        by_h = (by_a * scale + (along * (scale * scale * scale * (-1.0 / d))) * wide).astype(bf16)
        bwd_out[lax.rem(i, SENDS)] = (bwd_in[i].astype(f32) + by_h.astype(f32)).astype(bf16)

    def weights(i):
        number, rows = i // per, chunk(lax.rem(i, per))
        m, w = lax.rem(number, 2), lax.rem(number, held)
        for n, (left, right) in enumerate(((a_t.at[w], dg.at[m]), (a_t.at[w], du.at[m]), (dy_t.at[m], act.at[w]))):
            term = dot(left[rows, :], right[...]).astype(bf16).astype(f32)
            acc[n, rows, :] = jnp.where(number == 0, 0.0, acc[n, rows, :]) + term

    def half():
        m, w, mid = (micro - 1) % 2, (micro - 1) % held, tokens // 2
        for n, cols, left, right in tiles(a_t.at[w], dy_t.at[m], dg.at[m], du.at[m], act.at[w]):
            term = dot(left[:, :mid], right[:mid, cols])
            for q in range(d // ROWS):
                t_ring[(chunks + n * (d // ROWS) + q) % ring, :, cols] = term[q * ROWS:(q + 1) * ROWS]
        act_out[...] = act[w, mid:, :]
        a_out[...] = a_t[w, :, mid:]

    def step(i, carry):
        j = i - lag
        k = j - per
        forth, backwards = i < chunks, (j >= 0) & (j < chunks)

        @pl.when(last & forth)
        def _():
            onward(i).wait_recv()

            @pl.when(i >= SENDS)
            def _():
                back(i - SENDS).wait_send()
            gate_up(i, by_act)
            by_input(i)
            back(i).start()

        @pl.when(~last & forth)
        def _():
            forward_wait(i)
            gate_up(i)
            down(i)
            onward(i).start()

        @pl.when(first & (i == 2))
        def _():
            turn(wd_v, wd_t)

        @pl.when(~last & backwards)
        def _():
            back(j).wait_recv()

            @pl.when(~first & (j >= SENDS))
            def _():
                back(j - SENDS).wait_send()

            @pl.when(first)
            def _():
                by_gate_up(j)

            @pl.when(~first)
            def _():
                by_gate_up(j)
                by_input(j)
                back(j).start()

        ending = j >= chunks - per
        done = chunks - per
        low = jnp.where(ending, jnp.where(first, 2 * j - chunks, done - per), jnp.maximum(k, 0))
        high = jnp.where(ending, jnp.where(first, jnp.minimum(2 * j - chunks + 2, done), jnp.where(j == chunks - 1, done, 0)), k + 1)

        def share(n, c):
            weights(n)
            return c
        lax.fori_loop(low, high, share, 0)

        @pl.when(last & (i < chunks - 1))
        def _():
            by_hidden(i + 1)

        @pl.when(j == jnp.where(first, chunks - 2, chunks - 1))
        def _():
            half()
        return carry

    @pl.when(last)
    def _():
        by_hidden(0)

    @pl.when(first & (lax.rem(lax.axis_index("rep"), 2) == 0))
    def _():
        pl.delay(STAGGER)

    lax.fori_loop(0, chunks + max(LAGS), step, 0)

    for n in range(SENDS):
        @pl.when(~last)
        def _():
            onward(chunks - SENDS + n).wait_send()

        @pl.when(~first)
        def _():
            back(chunks - SENDS + n).wait_send()


def finish(m, chunks, acc, act, a_t, dg, du, dy_t, t_ring, out_g, out_u, out_d, stage, turned, sem):
    d, mid = acc.shape[1], act.shape[0]
    copies = []
    for p, (n, cols, left, right) in enumerate(tiles(a_t, dy_t.at[m, :, mid:], dg.at[m, mid:, :], du.at[m, mid:, :], act)):
        for q in range(d // ROWS):
            rows = slice(q * ROWS, (q + 1) * ROWS)
            term = t_ring[(chunks + n * (d // ROWS) + q) % t_ring.shape[0], :, cols] + dot(left[rows, :], right[:, cols])
            total = (acc[n, rows, cols] + term.astype(bf16).astype(f32)).astype(bf16)
            if n == 2:
                turned[cols, rows] = total.T
            else:
                stage[n, rows, cols] = total
        if n == 2:
            copy = pltpu.make_async_copy(turned.at[cols, :], out_d.at[0, cols, :], sem.at[p])
        else:
            copy = pltpu.make_async_copy(stage.at[n, :, cols], (out_g, out_u)[n].at[0, :, cols], sem.at[p])
        copy.start()
        copies.append(copy)
    for copy in copies:
        copy.wait()


def solution(mesh):
    stages = mesh.shape["pp"]

    def step(x, dy, wg, wu, wd):
        micro, tokens, d = x.shape
        ff = wg.shape[2]
        per = tokens // ROWS
        chunks = micro * per
        ring = max(LAGS) + 1
        held = pl.cdiv(ring - 1 + per, per) + 1
        hbm, vmem = pl.BlockSpec(memory_space=pl.ANY), pl.BlockSpec(memory_space=pltpu.VMEM)
        sums = pl.pallas_call(
            functools.partial(kernel, stages, micro, tokens),
            out_shape=(
                pltpu.VMEM((3, d, ff), f32),
                pltpu.VMEM((tokens // 2, ff), bf16),
                pltpu.VMEM((d, tokens // 2), bf16),
                pltpu.VMEM((2, tokens, ff), bf16),
                pltpu.VMEM((2, tokens, ff), bf16),
                pltpu.VMEM((2, d, tokens), bf16),
                pltpu.VMEM((ring, ROWS, ff), f32),
            ),
            in_specs=[hbm] * 5,
            out_specs=(vmem,) * 7,
            scratch_shapes=[
                pltpu.VMEM((chunks, ROWS, d), bf16),
                pltpu.VMEM((chunks, ROWS, d), bf16),
                pltpu.VMEM((SENDS, ROWS, d), bf16),
                pltpu.VMEM((SENDS, ROWS, d), bf16),
                pltpu.VMEM((ring, ROWS, ff), f32),
                pltpu.VMEM((ROWS, ff), bf16),
                pltpu.VMEM((held, tokens, ff), bf16),
                pltpu.VMEM((held, d, tokens), bf16),
                pltpu.VMEM((d, ff), bf16),
                pltpu.VMEM((d, ff), bf16),
                pltpu.VMEM((ff, d), bf16),
                pltpu.VMEM((ff, d), bf16),
                pltpu.VMEM((ff, d), bf16),
                pltpu.VMEM((d, ff), bf16),
                pltpu.SemaphoreType.DMA((chunks,)),
                pltpu.SemaphoreType.DMA((chunks,)),
                pltpu.SemaphoreType.DMA((SENDS,)),
                pltpu.SemaphoreType.DMA((SENDS,)),
                pltpu.SemaphoreType.DMA((3,)),
            ],
            compiler_params=pltpu.CompilerParams(collective_id=0, has_side_effects=True, vmem_limit_bytes=39 * 2**20),
        )(x, dy, wg, wu, wd)
        return pl.pallas_call(
            functools.partial(finish, (micro - 1) % 2, chunks),
            out_shape=(
                jax.ShapeDtypeStruct((1, d, ff), bf16),
                jax.ShapeDtypeStruct((1, d, ff), bf16),
                jax.ShapeDtypeStruct((1, ff, d), bf16),
            ),
            in_specs=[vmem] * 7,
            out_specs=(hbm,) * 3,
            scratch_shapes=[pltpu.VMEM((2, d, ff), bf16), pltpu.VMEM((ff, d), bf16), pltpu.SemaphoreType.DMA((3 * (ff // COLS),))],
            compiler_params=pltpu.CompilerParams(has_side_effects=True, vmem_limit_bytes=8 * 2**20),
        )(*sums)

    return jax.shard_map(
        step,
        mesh=mesh,
        in_specs=(P("rep", None, None),) * 2 + (P("pp", None, None),) * 3,
        out_specs=(P(("rep", "pp"), None, None),) * 3,
        check_vma=False,
    )
```

```python
import functools

import jax
import jax.numpy as jnp
from jax import lax
from jax.experimental import pallas as pl
from jax.experimental.pallas import tpu as pltpu
from jax.sharding import PartitionSpec as P

MESH = pl.DeviceIdType.MESH
ROWS = 128
COLS = 256
LAGS = (13,8,4,0)
LATE_LAGS = (13, 7, 3, 0)
STAGGER = 4000
SENDS = 3
f32, bf16 = jnp.float32, jnp.bfloat16


def dot(a, b):
    return jnp.dot(a, b, preferred_element_type=f32)


def chunk(c):
    return pl.ds(pl.multiple_of(c * ROWS, ROWS), ROWS)


def tiles(a_t, dy_t, dg, du, act):
    for n, left, right in ((2, dy_t, act), (0, a_t, dg), (1, a_t, du)):
        for t in range(0, right.shape[1], COLS):
            yield n, slice(t, t + COLS), left, right


def kernel(stages, micro, tokens, x, dy, wg, wu, wd,
           acc, act_out, a_out, dg, du, dy_t, t_ring,
           fwd_in, bwd_in, fwd_out, bwd_out, q_ring, by_act, act, a_t,
           wg_v, wu_v, wd_v, wg_t, wu_t, wd_t,
           fwd_sem, bwd_sem, fwd_send, bwd_send, w_sem):
    me = lax.axis_index("pp")
    per = tokens // ROWS
    chunks = micro * per
    d, ff = wg_v.shape
    ring, held = t_ring.shape[0], act.shape[0]
    first, last = me == 0, me == stages - 1
    late = lax.rem(lax.axis_index("rep"), 2) == 1
    lag = sum(jnp.where(me == n, jnp.where(late, a, b), 0) for n, (a, b) in enumerate(zip(LATE_LAGS, LAGS)))

    def load_x(i):
        return pltpu.make_async_copy(x.at[i // per, chunk(lax.rem(i, per)), :], fwd_in.at[i], fwd_sem.at[i])

    def load_dy(i):
        return pltpu.make_async_copy(dy.at[i // per, chunk(lax.rem(i, per)), :], bwd_in.at[i], bwd_sem.at[i])

    def onward(i):
        slot = lax.rem(i, SENDS)
        return pltpu.make_async_remote_copy(
            src_ref=fwd_out.at[slot], dst_ref=fwd_in.at[i], send_sem=fwd_send.at[slot], recv_sem=fwd_sem.at[i],
            device_id={"pp": me + 1}, device_id_type=MESH)

    def back(i):
        slot = lax.rem(i, SENDS)
        return pltpu.make_async_remote_copy(
            src_ref=bwd_out.at[slot], dst_ref=bwd_in.at[i], send_sem=bwd_send.at[slot], recv_sem=bwd_sem.at[i],
            device_id={"pp": me - 1}, device_id_type=MESH)

    loads = [pltpu.make_async_copy(src.at[0], dst, w_sem.at[n]) for n, (src, dst) in enumerate(((wg, wg_v), (wu, wu_v), (wd, wd_v)))]

    @pl.when(first)
    def _():
        load_x(0).start()
    for load in loads:
        load.start()

    @pl.when(first)
    def _():
        def go(i, c):
            load_x(i).start()
            return c
        lax.fori_loop(1, chunks, go, 0)

    @pl.when(last)
    def _():
        def go(i, c):
            load_dy(i).start()
            return c
        lax.fori_loop(0, chunks, go, 0)

    barrier = pltpu.get_barrier_semaphore()

    @pl.when(~first)
    def _():
        pl.semaphore_signal(barrier, inc=1, device_id={"pp": me - 1}, device_id_type=MESH)

    @pl.when(~last)
    def _():
        pl.semaphore_signal(barrier, inc=1, device_id={"pp": me + 1}, device_id_type=MESH)

    pl.semaphore_wait(barrier, jnp.where(first | last, 1, 2))

    for load in loads:
        load.wait()

    def turn(src, dst):
        def go(b, c):
            dst[:, chunk(b)] = src[chunk(b), :].T
            return c
        lax.fori_loop(0, src.shape[0] // ROWS, go, 0)

    @pl.when(~first)
    def _():
        turn(wd_v, wd_t)
        turn(wg_v, wg_t)
        turn(wu_v, wu_t)

    def norm(h):
        wide = h.astype(f32)
        scale = lax.rsqrt(jnp.sum(wide * wide, -1, keepdims=True) * (1.0 / d) + 1e-6)
        return wide, scale

    def forward_wait(i):
        @pl.when(first)
        def _():
            load_x(i).wait()

        @pl.when(~first)
        def _():
            onward(i).wait_recv()

        @pl.when(i >= SENDS)
        def _():
            onward(i - SENDS).wait_send()

    def gate_up(i, by_ref=None):
        slot, m, rows = lax.rem(i, ring), lax.rem(i // per, held), chunk(lax.rem(i, per))
        wide, scale = norm(fwd_in[i])
        a = (wide * scale).astype(bf16)
        a_t[m, :, rows] = a.T
        for t in range(0, ff, COLS):
            cols = slice(t, t + COLS)
            r, s = dot(a, wg_v[:, cols]), dot(a, wu_v[:, cols])
            v = 0.5 * jnp.tanh(0.5 * r) + 0.5
            silu = r * v
            slope = s * (v + silu * (1.0 - v))
            act[m, rows, cols] = (silu * s).astype(bf16)
            if by_ref is None:
                t_ring[slot, :, cols] = silu
                q_ring[slot, :, cols] = slope
            else:
                by = by_ref[:, cols].astype(f32)
                b = lax.rem(i // per, 2)
                du[b, rows, cols] = (silu * by).astype(bf16)
                dg[b, rows, cols] = (slope * by).astype(bf16)

    def down(i):
        m, rows = lax.rem(i // per, held), chunk(lax.rem(i, per))
        y = dot(act[m, rows, :], wd_v[...]).astype(bf16)
        fwd_out[lax.rem(i, SENDS)] = (fwd_in[i].astype(f32) + y.astype(f32)).astype(bf16)

    def by_hidden(i):
        load_dy(i).wait()
        by_y = bwd_in[i]
        dy_t[lax.rem(i // per, 2), :, chunk(lax.rem(i, per))] = by_y.T
        by_act[...] = dot(by_y, wd_t[...]).astype(bf16)

    def by_gate_up(i):
        slot, m, rows = lax.rem(i, ring), lax.rem(i // per, 2), chunk(lax.rem(i, per))
        by_y = bwd_in[i]
        dy_t[m, :, rows] = by_y.T
        for t in range(0, ff, COLS):
            cols = slice(t, t + COLS)
            by = dot(by_y, wd_t[:, cols]).astype(bf16).astype(f32)
            du[m, rows, cols] = (t_ring[slot, :, cols] * by).astype(bf16)
            dg[m, rows, cols] = (q_ring[slot, :, cols] * by).astype(bf16)

    def by_input(i):
        m, rows = lax.rem(i // per, 2), chunk(lax.rem(i, per))
        by_a = dot(du[m, rows, :], wu_t[...]).astype(bf16).astype(f32)
        by_a = (by_a + dot(dg[m, rows, :], wg_t[...]).astype(bf16).astype(f32)).astype(bf16).astype(f32)
        wide, scale = norm(fwd_in[i])
        along = jnp.sum(wide * by_a, -1, keepdims=True)
        by_h = (by_a * scale + (along * (scale * scale * scale * (-1.0 / d))) * wide).astype(bf16)
        bwd_out[lax.rem(i, SENDS)] = (bwd_in[i].astype(f32) + by_h.astype(f32)).astype(bf16)

    def weights(i):
        number, rows = i // per, chunk(lax.rem(i, per))
        m, w = lax.rem(number, 2), lax.rem(number, held)
        for n, (left, right) in enumerate(((a_t.at[w], dg.at[m]), (a_t.at[w], du.at[m]), (dy_t.at[m], act.at[w]))):
            term = dot(left[rows, :], right[...]).astype(bf16).astype(f32)
            acc[n, rows, :] = jnp.where(number == 0, 0.0, acc[n, rows, :]) + term

    def half():
        m, w, mid = (micro - 1) % 2, (micro - 1) % held, tokens // 2
        for n, cols, left, right in tiles(a_t.at[w], dy_t.at[m], dg.at[m], du.at[m], act.at[w]):
            term = dot(left[:, :mid], right[:mid, cols])
            for q in range(d // ROWS):
                t_ring[(chunks + n * (d // ROWS) + q) % ring, :, cols] = term[q * ROWS:(q + 1) * ROWS]
        act_out[...] = act[w, mid:, :]
        a_out[...] = a_t[w, :, mid:]

    def step(i, carry):
        j = i - lag
        k = j - per
        forth, backwards = i < chunks, (j >= 0) & (j < chunks)

        @pl.when(last & forth)
        def _():
            onward(i).wait_recv()

            @pl.when(i >= SENDS)
            def _():
                back(i - SENDS).wait_send()
            gate_up(i, by_act)
            by_input(i)
            back(i).start()

        @pl.when(~last & forth)
        def _():
            forward_wait(i)
            gate_up(i)
            down(i)
            onward(i).start()

        @pl.when(first & (i == 2))
        def _():
            turn(wd_v, wd_t)

        @pl.when(~last & backwards)
        def _():
            back(j).wait_recv()

            @pl.when(~first & (j >= SENDS))
            def _():
                back(j - SENDS).wait_send()

            @pl.when(first)
            def _():
                by_gate_up(j)

            @pl.when(~first)
            def _():
                by_gate_up(j)
                by_input(j)
                back(j).start()

        ending = j >= chunks - per
        done = chunks - per
        low = jnp.where(ending, jnp.where(first, 2 * j - chunks, done - per), jnp.maximum(k, 0))
        high = jnp.where(ending, jnp.where(first, jnp.minimum(2 * j - chunks + 2, done), jnp.where(j == chunks - 1, done, 0)), k + 1)

        def share(n, c):
            weights(n)
            return c
        lax.fori_loop(low, high, share, 0)

        @pl.when(last & (i < chunks - 1))
        def _():
            by_hidden(i + 1)

        @pl.when(j == jnp.where(first, chunks - 2, chunks - 1))
        def _():
            half()
        return carry

    @pl.when(last)
    def _():
        by_hidden(0)

    @pl.when(first & late)
    def _():
        pl.delay(STAGGER)

    lax.fori_loop(0, chunks + max(LAGS), step, 0)

    for n in range(SENDS):
        @pl.when(~last)
        def _():
            onward(chunks - SENDS + n).wait_send()

        @pl.when(~first)
        def _():
            back(chunks - SENDS + n).wait_send()


def finish(m, chunks, acc, act, a_t, dg, du, dy_t, t_ring, out_g, out_u, out_d, stage, turned, sem):
    d, mid = acc.shape[1], act.shape[0]
    copies = []
    for p, (n, cols, left, right) in enumerate(tiles(a_t, dy_t.at[m, :, mid:], dg.at[m, mid:, :], du.at[m, mid:, :], act)):
        for q in range(d // ROWS):
            rows = slice(q * ROWS, (q + 1) * ROWS)
            term = t_ring[(chunks + n * (d // ROWS) + q) % t_ring.shape[0], :, cols] + dot(left[rows, :], right[:, cols])
            total = (acc[n, rows, cols] + term.astype(bf16).astype(f32)).astype(bf16)
            if n == 2:
                turned[cols, rows] = total.T
            else:
                stage[n, rows, cols] = total
        if n == 2:
            copy = pltpu.make_async_copy(turned.at[cols, :], out_d.at[0, cols, :], sem.at[p])
        else:
            copy = pltpu.make_async_copy(stage.at[n, :, cols], (out_g, out_u)[n].at[0, :, cols], sem.at[p])
        copy.start()
        copies.append(copy)
    for copy in copies:
        copy.wait()


def solution(mesh):
    stages = mesh.shape["pp"]

    def step(x, dy, wg, wu, wd):
        micro, tokens, d = x.shape
        ff = wg.shape[2]
        per = tokens // ROWS
        chunks = micro * per
        ring = max(LAGS) + 1
        held = pl.cdiv(ring - 1 + per, per) + 1
        hbm, vmem = pl.BlockSpec(memory_space=pl.ANY), pl.BlockSpec(memory_space=pltpu.VMEM)
        sums = pl.pallas_call(
            functools.partial(kernel, stages, micro, tokens),
            out_shape=(
                pltpu.VMEM((3, d, ff), f32),
                pltpu.VMEM((tokens // 2, ff), bf16),
                pltpu.VMEM((d, tokens // 2), bf16),
                pltpu.VMEM((2, tokens, ff), bf16),
                pltpu.VMEM((2, tokens, ff), bf16),
                pltpu.VMEM((2, d, tokens), bf16),
                pltpu.VMEM((ring, ROWS, ff), f32),
            ),
            in_specs=[hbm] * 5,
            out_specs=(vmem,) * 7,
            scratch_shapes=[
                pltpu.VMEM((chunks, ROWS, d), bf16),
                pltpu.VMEM((chunks, ROWS, d), bf16),
                pltpu.VMEM((SENDS, ROWS, d), bf16),
                pltpu.VMEM((SENDS, ROWS, d), bf16),
                pltpu.VMEM((ring, ROWS, ff), f32),
                pltpu.VMEM((ROWS, ff), bf16),
                pltpu.VMEM((held, tokens, ff), bf16),
                pltpu.VMEM((held, d, tokens), bf16),
                pltpu.VMEM((d, ff), bf16),
                pltpu.VMEM((d, ff), bf16),
                pltpu.VMEM((ff, d), bf16),
                pltpu.VMEM((ff, d), bf16),
                pltpu.VMEM((ff, d), bf16),
                pltpu.VMEM((d, ff), bf16),
                pltpu.SemaphoreType.DMA((chunks,)),
                pltpu.SemaphoreType.DMA((chunks,)),
                pltpu.SemaphoreType.DMA((SENDS,)),
                pltpu.SemaphoreType.DMA((SENDS,)),
                pltpu.SemaphoreType.DMA((3,)),
            ],
            compiler_params=pltpu.CompilerParams(collective_id=0, has_side_effects=True, vmem_limit_bytes=39 * 2**20),
        )(x, dy, wg, wu, wd)
        return pl.pallas_call(
            functools.partial(finish, (micro - 1) % 2, chunks),
            out_shape=(
                jax.ShapeDtypeStruct((1, d, ff), bf16),
                jax.ShapeDtypeStruct((1, d, ff), bf16),
                jax.ShapeDtypeStruct((1, ff, d), bf16),
            ),
            in_specs=[vmem] * 7,
            out_specs=(hbm,) * 3,
            scratch_shapes=[pltpu.VMEM((2, d, ff), bf16), pltpu.VMEM((ff, d), bf16), pltpu.SemaphoreType.DMA((3 * (ff // COLS),))],
            compiler_params=pltpu.CompilerParams(has_side_effects=True, vmem_limit_bytes=8 * 2**20),
        )(*sums)

    return jax.shard_map(
        step,
        mesh=mesh,
        in_specs=(P("rep", None, None),) * 2 + (P("pp", None, None),) * 3,
        out_specs=(P(("rep", "pp"), None, None),) * 3,
        check_vma=False,
    )
```
